8 devices in a mesh: dp: 2 (over z, y), sp: 4 (over x, core).
Axes of the slice: x: 2, y: 2, z: 1, core: 2. Of those that a mesh axis runs over, the one named last changes fastest.
Arguments:
- hidden_states: bfloat16 [12, 384, 2304], P('dp', 'sp'), parts along dimension 0
- positions: int32 [12, 384], P('dp', 'sp'), parts along dimension 0
- gain_attn: float32 [8, 2304], replicated
- gain_mlp: float32 [8, 2304], replicated
- w_query: bfloat16 [8, 2304, 8, 256], replicated
- w_key: bfloat16 [8, 2304, 4, 256], replicated
- w_value: bfloat16 [8, 2304, 4, 256], replicated
- w_out: bfloat16 [8, 8, 256, 2304], replicated
- w_gate: bfloat16 [8, 2304, 9216], replicated
- w_up: bfloat16 [8, 2304, 9216], replicated
- w_down: bfloat16 [8, 9216, 2304], replicated
Outputs:
- output: bfloat16 [12, 384, 2304], P('dp', 'sp'), parts along dimension 0
There are 2 independent parts. The reference program is written for one: setup_inputs(seed, part) draws one part's arguments, and reference() takes and returns one part's arrays. A program takes and returns all parts, laid end to end along the dimension named above; an argument that names none is the same for every part.
All inputs are finite; a program needn't handle non-finite values.
Results may differ from the reference program's by a relative error of at most 0.0175564.
Values are sent between devices in bfloat16 or wider.
A program may use at most 4.75 GiB of HBM per device.

```python
import jax
import jax.numpy as jnp
from jax import lax

D_MODEL = 2304
HEADS = 8
KV_HEADS = 4
HEAD_DIM = 256
FF_DIM = 9216
LAYERS = 8
BATCH = 6
SEQ_DEV = 96
SEQ_LEN = 384
WINDOW = 144

EPSILON = 1e-5
THETA = 10000.0


def setup_inputs(seed: int = 0, part: int = 0) -> dict:
    root_key = jax.random.key(seed)
    shared_key, group_root = jax.random.split(root_key)
    group_key = jax.random.fold_in(group_root, part)
    key_hidden, key_offset, key_step = jax.random.split(group_key, 3)
    weight_keys = jax.random.split(shared_key, 9)
    hidden_states = jax.random.normal(key_hidden, (BATCH, SEQ_LEN, D_MODEL), jnp.float32).astype(jnp.bfloat16)
    offsets = jax.random.randint(key_offset, (BATCH, 1), 0, SEQ_LEN)
    increments = jax.random.randint(key_step, (BATCH, SEQ_LEN), 1, 3)
    positions = (offsets + jnp.cumsum(increments, axis=1)).astype(jnp.int32)
    out_scale = (WINDOW / (3.0 * HEADS * HEAD_DIM)) ** 0.5

    def draw_weight(key, shape, scale):
        return (jax.random.normal(key, shape, jnp.float32) * scale).astype(jnp.bfloat16)

    return {
        'hidden_states': hidden_states,
        'positions': positions,
        'gain_attn': jax.random.uniform(weight_keys[0], (LAYERS, D_MODEL), jnp.float32, 0.5, 1.5),
        'gain_mlp': jax.random.uniform(weight_keys[1], (LAYERS, D_MODEL), jnp.float32, 0.5, 1.5),
        'w_query': draw_weight(weight_keys[2], (LAYERS, D_MODEL, HEADS, HEAD_DIM), D_MODEL ** -0.5),
        'w_key': draw_weight(weight_keys[3], (LAYERS, D_MODEL, KV_HEADS, HEAD_DIM), D_MODEL ** -0.5),
        'w_value': draw_weight(weight_keys[4], (LAYERS, D_MODEL, KV_HEADS, HEAD_DIM), D_MODEL ** -0.5),
        'w_out': draw_weight(weight_keys[5], (LAYERS, HEADS, HEAD_DIM, D_MODEL), out_scale),
        'w_gate': draw_weight(weight_keys[6], (LAYERS, D_MODEL, FF_DIM), D_MODEL ** -0.5),
        'w_up': draw_weight(weight_keys[7], (LAYERS, D_MODEL, FF_DIM), D_MODEL ** -0.5),
        'w_down': draw_weight(weight_keys[8], (LAYERS, FF_DIM, D_MODEL), (2.0 / FF_DIM) ** 0.5),
    }


def rms_norm(values, gain):
    as_float = values.astype(jnp.float32)
    inv_rms = lax.rsqrt(jnp.mean(as_float * as_float, axis=-1, keepdims=True) + EPSILON)
    return (as_float * inv_rms * gain).astype(jnp.bfloat16)


def rotary(values, cos_t, sin_t):
    half_dim = values.shape[-1] // 2
    lower_part = values[..., :half_dim]
    upper_part = values[..., half_dim:]
    return jnp.concatenate([lower_part * cos_t - upper_part * sin_t, upper_part * cos_t + lower_part * sin_t], axis=-1)


def reference(hidden_states, positions, gain_attn, gain_mlp, w_query, w_key, w_value, w_out, w_gate, w_up, w_down):
    n_blocks = SEQ_LEN // SEQ_DEV
    group_size = HEADS // KV_HEADS
    ctx_len = 3 * SEQ_DEV
    half_dim = HEAD_DIM // 2
    inv_freq = THETA ** (-(jnp.arange(half_dim, dtype=jnp.float32) * 2.0) / HEAD_DIM)
    pos_blocks = jnp.swapaxes(positions.reshape(BATCH, n_blocks, SEQ_DEV), 0, 1)
    angles = pos_blocks.astype(jnp.float32)[..., None] * inv_freq
    cos_all = jnp.cos(angles)[:, :, :, None, :]
    sin_all = jnp.sin(angles)[:, :, :, None, :]
    x_blocks = jnp.swapaxes(hidden_states.reshape(BATCH, n_blocks, SEQ_DEV, D_MODEL), 0, 1)
    q_index = jnp.arange(SEQ_DEV)[:, None]
    k_index = jnp.arange(ctx_len)[None, :]
    distance = q_index + 2 * SEQ_DEV - k_index
    band = (distance >= 0) & (distance < WINDOW)
    kv_pad = jnp.zeros((2, BATCH, SEQ_DEV, KV_HEADS, HEAD_DIM), jnp.bfloat16)

    def layer_step(hidden, params):
        attn_gain, mlp_gain, q_weight, k_weight, v_weight, o_weight, gate_weight, up_weight, down_weight = params
        q_weight = q_weight.astype(jnp.float32)
        k_weight = k_weight.astype(jnp.float32)
        v_weight = v_weight.astype(jnp.float32)
        o_weight = o_weight.astype(jnp.float32)
        gate_weight = gate_weight.astype(jnp.float32)
        up_weight = up_weight.astype(jnp.float32)
        down_weight = down_weight.astype(jnp.float32)

        def project(block):
            x_blk, cos_t, sin_t = block
            normed = rms_norm(x_blk, attn_gain).astype(jnp.float32)
            queries = rotary(jnp.einsum('btd,dhe->bthe', normed, q_weight), cos_t, sin_t)
            keys = rotary(jnp.einsum('btd,dhe->bthe', normed, k_weight), cos_t, sin_t)
            values = jnp.einsum('btd,dhe->bthe', normed, v_weight)
            return queries.astype(jnp.bfloat16), keys.astype(jnp.bfloat16), values.astype(jnp.bfloat16)

        q_all, k_all, v_all = lax.map(project, (hidden, cos_all, sin_all))
        k_pad = jnp.concatenate([kv_pad, k_all], axis=0)
        v_pad = jnp.concatenate([kv_pad, v_all], axis=0)

        def finish(block):
            block_idx, x_blk, q_blk = block
            k_ctx = jnp.swapaxes(lax.dynamic_slice_in_dim(k_pad, block_idx, 3, axis=0), 0, 1).reshape(BATCH, ctx_len, KV_HEADS, HEAD_DIM)
            v_ctx = jnp.swapaxes(lax.dynamic_slice_in_dim(v_pad, block_idx, 3, axis=0), 0, 1).reshape(BATCH, ctx_len, KV_HEADS, HEAD_DIM)
            q_grouped = q_blk.reshape(BATCH, SEQ_DEV, KV_HEADS, group_size, HEAD_DIM)
            scores = jnp.einsum('bqhgd,bkhd->bhgqk', q_grouped.astype(jnp.float32), k_ctx.astype(jnp.float32)) * HEAD_DIM ** -0.5
            valid = band & (k_index >= (2 - block_idx) * SEQ_DEV)
            scores = jnp.where(valid, scores, -jnp.inf)
            attn_probs = jax.nn.softmax(scores, axis=-1).astype(jnp.bfloat16)
            attn_vals = jnp.einsum('bhgqk,bkhd->bqhgd', attn_probs.astype(jnp.float32), v_ctx.astype(jnp.float32)).astype(jnp.bfloat16)
            attn_vals = attn_vals.reshape(BATCH, SEQ_DEV, HEADS, HEAD_DIM)
            attn_proj = jnp.einsum('bqhe,hed->bqd', attn_vals.astype(jnp.float32), o_weight)
            mid_hidden = (x_blk.astype(jnp.float32) + attn_proj).astype(jnp.bfloat16)
            normed = rms_norm(mid_hidden, mlp_gain).astype(jnp.float32)
            gate_proj = jnp.einsum('btd,df->btf', normed, gate_weight)
            up_proj = jnp.einsum('btd,df->btf', normed, up_weight)
            activated = (jax.nn.silu(gate_proj) * up_proj).astype(jnp.bfloat16)
            down_proj = jnp.einsum('btf,fd->btd', activated.astype(jnp.float32), down_weight)
            return (mid_hidden.astype(jnp.float32) + down_proj).astype(jnp.bfloat16)

        new_hidden = lax.map(finish, (jnp.arange(n_blocks), hidden, q_all))
        return new_hidden, None

    final_hidden, _ = lax.scan(layer_step, x_blocks, (gain_attn, gain_mlp, w_query, w_key, w_value, w_out, w_gate, w_up, w_down))
    return jnp.swapaxes(final_hidden, 0, 1).reshape(BATCH, SEQ_LEN, D_MODEL)
```

```python
import functools

import jax
import jax.numpy as jnp
from jax import lax
from jax.experimental import pallas as pl
from jax.experimental.pallas import tpu as pltpu
from jax.sharding import PartitionSpec as P

EPSILON = 1e-5
THETA = 10000.0
LAYERS, D, HEADS, KV, HD, FF = 8, 2304, 8, 4, 256, 9216
SEQ, HALF = 384, 192
ROWS = SEQ + HALF
WINDOW = 144
PAD = 160
QB = 96
CTX = PAD + QB
WHOLE_KEYS = PAD + SEQ
KEYS = WHOLE_KEYS + PAD + HALF
FC = 512
NF = FF // FC
GW = 256
KC = 1024
NO, ND = HEADS * HD // KC, FF // KC
SLAB = 128
NS = D // SLAB
NB = 192
NW = D // 3
WREL = 2 * KV * HD + HEADS * HD
MESH = pl.DeviceIdType.MESH
F32, BF16 = jnp.float32, jnp.bfloat16


def dot(a, b):
    return jnp.dot(a, b, preferred_element_type=F32)


def rope_tables(positions):
    half = HD // 2
    inv_freq = THETA ** (-(jnp.arange(half, dtype=F32) * 2.0) / HD)
    angles = positions.astype(F32)[:, None] * inv_freq
    return jnp.cos(angles), jnp.sin(angles)


def stack_kernel(x_hbm, cos_ref, sin_ref, ga_ref, gm_ref, wq, wk, wv, wo, wg, wu, wd, out_hbm,
                 x, h, wrel, q, k, v, acc, bias, rq, rk, rv, gb, ub, db,
                 sx, sq, sk, sv, sg, su, sd, send_sem, recv_sem, credit):
    me = lax.axis_index('sp')
    core = lax.rem(me, 2)
    partner = {'sp': me + 1 - 2 * core}

    def slab_copies(l, i):
        s = lax.rem(l * NS + i, 2)
        rows = pl.ds(i * SLAB, SLAB)
        return (pltpu.make_async_copy(wq.at[l, rows], rq.at[s], sq.at[s]),
                pltpu.make_async_copy(wk.at[l, rows], rk.at[s], sk.at[s]),
                pltpu.make_async_copy(wv.at[l, rows], rv.at[s], sv.at[s]))

    def gate_copies(l, i):
        s = lax.rem(i, 2)
        cols = pl.ds(i * FC, FC)
        return (pltpu.make_async_copy(wg.at[l, :, cols], gb.at[s], sg.at[s]),
                pltpu.make_async_copy(wu.at[l, :, cols], ub.at[s], su.at[s]))

    def out_copies(l, i):
        s = lax.rem(l * (NO + ND) + i, 2)
        return (pltpu.make_async_copy(wo.at[l, pl.ds(i * KC, KC)], db.at[s], sd.at[s]),)

    def down_copies(l, i):
        s = lax.rem(l * (NO + ND) + NO + i, 2)
        return (pltpu.make_async_copy(wd.at[l, pl.ds(i * KC, KC)], db.at[s], sd.at[s]),)

    def start(copies):
        for c in copies:
            c.start()

    def wait(copies):
        for c in copies:
            c.wait()

    def rms_norm(gain_ref, l):
        gain = gain_ref[pl.ds(l, 1), :]

        def block(b, _):
            rows = pl.ds(pl.multiple_of(b * NB, NB), NB)
            xf = x[rows].astype(F32)
            inv = lax.rsqrt(jnp.mean(xf * xf, axis=-1, keepdims=True) + EPSILON)
            h[rows] = (xf * inv * gain).astype(BF16)
            return 0

        lax.fori_loop(0, ROWS // NB, block, 0)

    def rotated(t):
        cos_t, sin_t = cos_ref[...], sin_ref[...]
        a, b = t[:, :HD // 2], t[:, HD // 2:]
        return jnp.concatenate([a * cos_t - b * sin_t, b * cos_t + a * sin_t], axis=-1).astype(BF16)

    def store_keys(ref, head, t):
        ref[head, PAD:WHOLE_KEYS] = t[:SEQ]
        ref[head, WHOLE_KEYS + PAD:KEYS] = t[SEQ:]

    def halo_copies():
        src, dst = pl.ds(KEYS - PAD, PAD), pl.ds(WHOLE_KEYS, PAD)
        return [pltpu.make_async_remote_copy(
            src_ref=ref.at[:, src], dst_ref=ref.at[:, dst], send_sem=send_sem.at[n], recv_sem=recv_sem.at[n],
            device_id=partner, device_id_type=MESH) for n, ref in enumerate((k, v))]

    def attend(q_row, key_row, variant):
        mask = bias[variant]
        for g in range(KV):
            qs = jnp.concatenate([q[2 * g, pl.ds(q_row, QB)], q[2 * g + 1, pl.ds(q_row, QB)]], axis=0)
            kc, vc = k[g, pl.ds(key_row, CTX)], v[g, pl.ds(key_row, CTX)]
            s = lax.dot_general(qs, kc, (((1,), (1,)), ((), ())), preferred_element_type=F32)
            s = s * HD ** -0.5 + jnp.concatenate([mask, mask], axis=0)
            e = jnp.exp(s - jnp.max(s, axis=-1, keepdims=True))
            p = (e * (1.0 / jnp.sum(e, axis=-1, keepdims=True))).astype(BF16)
            o = dot(p, vc).astype(BF16)
            q[2 * g, pl.ds(q_row, QB)] = o[:QB]
            q[2 * g + 1, pl.ds(q_row, QB)] = o[QB:]

    barrier = pltpu.get_barrier_semaphore()
    pl.semaphore_signal(barrier, inc=1, device_id=partner, device_id_type=MESH)
    pl.semaphore_wait(barrier, 1)

    x_in = pltpu.make_async_copy(x_hbm, x, sx)
    x_in.start()
    start(slab_copies(0, 0))
    start(slab_copies(0, 1))
    start(out_copies(0, 0))
    start(out_copies(0, 1))
    start(gate_copies(0, 0))
    start(gate_copies(0, 1))

    k[:, 0:PAD] = jnp.zeros((KV, PAD, HD), BF16)
    v[:, 0:PAD] = jnp.zeros((KV, PAD, HD), BF16)
    row = lax.broadcasted_iota(jnp.int32, (QB, CTX), 0)
    col = lax.broadcasted_iota(jnp.int32, (QB, CTX), 1)
    distance = row + PAD - col
    band = (distance >= 0) & (distance < WINDOW)
    for n, first in enumerate((PAD, PAD - QB, 0)):
        bias[n] = jnp.where(band & (col >= first), 0.0, -jnp.inf).astype(F32)
    x_in.wait()

    def layer(l, _):
        rms_norm(ga_ref, l)

        def relayout(i, _):
            s = lax.rem(l * NS + i, 2)
            wait(slab_copies(l, i))
            rows = pl.ds(pl.multiple_of(i * SLAB, SLAB), SLAB)
            wrel[rows, 0:KV * HD] = pltpu.einshape("dhe->d(he)", rk[s])
            wrel[rows, KV * HD:2 * KV * HD] = pltpu.einshape("dhe->d(he)", rv[s])
            wrel[rows, 2 * KV * HD:] = pltpu.einshape("dhe->d(he)", rq[s])

            @pl.when(i + 2 < NS)
            def _():
                start(slab_copies(l, i + 2))

            @pl.when((i + 2 >= NS) & (l + 1 < LAYERS))
            def _():
                start(slab_copies(l + 1, i + 2 - NS))
            return 0

        lax.fori_loop(0, NS, relayout, 0)

        def key_step(i, _):
            t = dot(h[...], wrel[:, pl.ds(pl.multiple_of(i * 2 * HD, 2 * HD), 2 * HD)])
            for j in range(2):
                store_keys(k, 2 * i + j, rotated(t[:, j * HD:(j + 1) * HD]))
            return 0

        def value_step(i, _):
            t = dot(h[...], wrel[:, pl.ds(pl.multiple_of((KV + 2 * i) * HD, 2 * HD), 2 * HD)])
            for j in range(2):
                store_keys(v, 2 * i + j, t[:, j * HD:(j + 1) * HD].astype(BF16))
            return 0

        def query_step(i, _):
            t = dot(h[...], wrel[:, pl.ds(pl.multiple_of((2 * KV + 2 * i) * HD, 2 * HD), 2 * HD)])
            for j in range(2):
                q[2 * i + j] = rotated(t[:, j * HD:(j + 1) * HD])
            return 0

        lax.fori_loop(0, KV // 2, key_step, 0)
        lax.fori_loop(0, KV // 2, value_step, 0)

        @pl.when(l > 0)
        def _():
            pl.semaphore_wait(credit, 1)

        halo = halo_copies()
        start(halo)
        lax.fori_loop(0, HEADS // 2, query_step, 0)

        def whole_step(b, _):
            r = pl.multiple_of(b * QB, QB)
            attend(r, r, jnp.minimum(b, 2))
            return 0

        def half_step(b, _):
            r = pl.multiple_of(b * QB, QB)
            attend(SEQ + r, WHOLE_KEYS + r, b + (2 - b) * core)
            return 0

        lax.fori_loop(0, SEQ // QB, whole_step, 0)
        wait(halo)
        lax.fori_loop(0, HALF // QB, half_step, 0)

        @pl.when(l + 1 < LAYERS)
        def _():
            pl.semaphore_signal(credit, inc=1, device_id=partner, device_id_type=MESH)

        acc[...] = x[...].astype(F32)

        def out_step(i, _):
            wait(out_copies(l, i))
            s = lax.rem(l * (NO + ND) + i, 2)
            heads = KC // HD
            o = jnp.concatenate([q[heads * i + j] for j in range(heads)], axis=1)
            for n in range(0, D, NW):
                acc[:, n:n + NW] += dot(o, db[s, :, n:n + NW])
            start(down_copies(l, i))
            return 0

        lax.fori_loop(0, NO, out_step, 0)
        x[...] = acc[...].astype(BF16)
        rms_norm(gm_ref, l)

        def gate_step(i, _):
            wait(gate_copies(l, i))
            s = lax.rem(i, 2)
            per = WREL // FC
            rows = pl.ds(pl.multiple_of((i // per) * ROWS, ROWS), ROWS)
            first = lax.rem(i, per) * FC
            for n in range(0, FC, GW):
                g = dot(h[...], gb[s, :, n:n + GW])
                u = dot(h[...], ub[s, :, n:n + GW])
                wrel[rows, pl.ds(pl.multiple_of(first + n, GW), GW)] = (g * (1.0 / (1.0 + jnp.exp(-g))) * u).astype(BF16)

            @pl.when(i + 2 < NF)
            def _():
                start(gate_copies(l, i + 2))

            @pl.when((i + 2 >= NF) & (l + 1 < LAYERS))
            def _():
                start(gate_copies(l + 1, i + 2 - NF))
            return 0

        lax.fori_loop(0, NF, gate_step, 0)
        acc[...] = x[...].astype(F32)

        def down_step(i, _):
            wait(down_copies(l, i))
            s = lax.rem(l * (NO + ND) + NO + i, 2)
            per = WREL // KC
            rows = pl.ds(pl.multiple_of((i // per) * ROWS, ROWS), ROWS)
            cols = pl.ds(pl.multiple_of(lax.rem(i, per) * KC, KC), KC)
            for n in range(0, D, NW):
                acc[:, n:n + NW] += dot(wrel[rows, cols], db[s, :, n:n + NW])

            @pl.when(i + 2 < ND)
            def _():
                start(down_copies(l, i + 2))

            @pl.when((i + 2 >= ND) & (l + 1 < LAYERS))
            def _():
                start(out_copies(l + 1, i + 2 - ND))
            return 0

        lax.fori_loop(0, ND, down_step, 0)
        x[...] = acc[...].astype(BF16)
        return 0

    lax.fori_loop(0, LAYERS, layer, 0)
    x_out = pltpu.make_async_copy(x, out_hbm, sx)
    x_out.start()
    x_out.wait()


def run_stack(x, cos_t, sin_t, *weights):
    vmem, hbm = pl.BlockSpec(memory_space=pltpu.VMEM), pl.BlockSpec(memory_space=pltpu.HBM)
    dma = pltpu.SemaphoreType.DMA
    return pl.pallas_call(
        stack_kernel,
        out_shape=jax.ShapeDtypeStruct((ROWS, D), BF16),
        in_specs=[hbm] + [vmem] * 4 + [hbm] * 7,
        out_specs=hbm,
        scratch_shapes=[
            pltpu.VMEM((ROWS, D), BF16),
            pltpu.VMEM((ROWS, D), BF16),
            pltpu.VMEM((D, WREL), BF16),
            pltpu.VMEM((HEADS, ROWS, HD), BF16),
            pltpu.VMEM((KV, KEYS, HD), BF16),
            pltpu.VMEM((KV, KEYS, HD), BF16),
            pltpu.VMEM((ROWS, D), F32),
            pltpu.VMEM((3, QB, CTX), F32),
            pltpu.VMEM((2, SLAB, HEADS, HD), BF16),
            pltpu.VMEM((2, SLAB, KV, HD), BF16),
            pltpu.VMEM((2, SLAB, KV, HD), BF16),
            pltpu.VMEM((2, D, FC), BF16),
            pltpu.VMEM((2, D, FC), BF16),
            pltpu.VMEM((2, KC, D), BF16),
            dma, dma((2,)), dma((2,)), dma((2,)), dma((2,)), dma((2,)), dma((2,)),
            dma((2,)), dma((2,)), pltpu.SemaphoreType.REGULAR,
        ],
        compiler_params=pltpu.CompilerParams(
            vmem_limit_bytes=67043328, collective_id=0, has_side_effects=True),
        name='decoder_stack',
    )(x, cos_t, sin_t, *weights)


def half_perm(r):
    return [(2 * x + c, 2 * (c ^ r) + x) for x in range(2) for c in range(2)]


def to_sequences(blocks, core):
    whole = lax.all_to_all(jnp.stack([blocks[0], blocks[2], blocks[3], blocks[5]]), 'sp', 0, 0)
    flip = lax.axis_index('sp') >= 2
    first = lax.ppermute(jnp.where(core == 0, blocks[1], blocks[4]), 'sp', half_perm(0))
    second = lax.ppermute(jnp.where(core == 0, blocks[4], blocks[1]), 'sp', half_perm(1))
    low, high = jnp.where(flip, second, first), jnp.where(flip, first, second)
    return jnp.concatenate([whole.reshape(SEQ, -1), low, high], axis=0)


def to_shards(rows, core):
    blocks = rows.reshape(ROWS // QB, QB, -1)
    whole = lax.all_to_all(blocks[:4], 'sp', 0, 0)
    flip = lax.axis_index('sp') >= 2
    inverse = [[(b, a) for a, b in half_perm(r)] for r in range(2)]
    first = lax.ppermute(jnp.where(flip, blocks[5], blocks[4]), 'sp', inverse[0])
    second = lax.ppermute(jnp.where(flip, blocks[4], blocks[5]), 'sp', inverse[1])
    one, four = jnp.where(core == 0, first, second), jnp.where(core == 0, second, first)
    return jnp.stack([whole[0], one, whole[1], whole[2], four, whole[3]])


def solution(mesh):
    def local_stack(hidden_states, positions, gain_attn, gain_mlp, w_query, w_key, w_value, w_out, w_gate, w_up, w_down):
        core = lax.rem(lax.axis_index('sp'), 2)
        every = lax.all_gather(positions, 'sp', axis=1, tiled=True)
        chip = lax.axis_index('sp') // 2
        whole_pos = lax.dynamic_slice_in_dim(every, 3 * chip + 2 * core, 1, axis=0)[0]
        half_pos = lax.dynamic_slice(every, (3 * chip + 1, HALF * core), (1, HALF))[0]
        cos_t, sin_t = rope_tables(jnp.concatenate([whole_pos, half_pos]))
        x = to_sequences(hidden_states, core)
        out = run_stack(x, cos_t, sin_t, gain_attn, gain_mlp, w_query, w_key, w_value,
                        w_out.reshape(LAYERS, HEADS * HD, D), w_gate, w_up, w_down)
        return to_shards(out, core)

    row_spec = P('dp', 'sp', None)
    return jax.shard_map(local_stack, mesh=mesh, in_specs=(row_spec, P('dp', 'sp'), P(), P(), P(), P(), P(), P(), P(), P(), P()), out_specs=row_spec, check_vma=False)
```
